256 devices in a mesh: ta: 16 (over x, z_hi, core), gz: 4 (over y), gy: 4 (over z_lo).
Axes of the slice: x: 4, y: 4, z: 8 (z_hi: 2, z_lo: 4; z = z_hi * 4 + z_lo), core: 2. Of those that a mesh axis runs over, the one named last changes fastest.
Arguments:
- near_null: float32 [64, 16, 16, 12, 12, 128], P('ta', 'gz', 'gy'), may hold values from -400 to 400
- offsets: int32 [4], replicated, may hold values from 1 to 3
- owner_slot: int32 [16, 4, 4, 16], P('ta', 'gz', 'gy'), may hold values from 0 to 15, each once within a row
Outputs:
- result: float32 [4096, 2, 12, 6, 2, 256], P(('ta', 'gz', 'gy'))
The draws below stay inside these ranges and needn't reach their ends.
Inputs may be any that keep to these rules, and one draw needn't show every extreme that they name: The same offsets hold for every device. `owner_slot`: each device's row is a permutation of 0 to 15.
All inputs are finite; a program needn't handle non-finite values.
Results may differ from the reference program's by a relative error of at most 0.0001.
Values sent between devices are 32-bit elements; how exact they have to be, the bound alone decides.
A program may use at most 256 MiB of HBM per device.

```python
import jax
import jax.numpy as jnp
from jax import lax

V = 12
C = 12
AGG = 4
NX = 64
NT = 64
NZ = 16
NY = 16
NAGG = 16
N_TA = 16
N_GZ = 4
N_GY = 4


def draw_near_null(key, part):
    key_base, key_site, key_vector = jax.random.split(key, 3)
    shape = (NT, NZ, NY, V, C, 2 * NX)
    site_scale = jnp.exp(jax.random.uniform(key_site, (NT, NZ, NY, 1, 1, 2 * NX), jnp.float32) * jnp.log(10.0))
    vector_scale = jnp.exp(jax.random.uniform(key_vector, (1, 1, 1, V, 1, 1), jnp.float32) * jnp.log(10.0))
    base = jnp.clip(jax.random.normal(key_base, shape, jnp.float32), -4.0, 4.0)
    return (base * site_scale * vector_scale).astype(jnp.float32)


def with_ends(entries, rng, smallest, high):
    longest = entries.shape.index(max(entries.shape))
    spots = []
    for shift in (0, 1):
        where = [jax.random.randint(jax.random.fold_in(rng, axis), (), 0, length) for axis, length in enumerate(entries.shape)]
        where[longest] = (where[longest] + shift) % entries.shape[longest]
        spots.append(tuple(where))
    return entries.at[spots[0]].set(smallest).at[spots[1]].set(high)


def setup_inputs(seed: int = 0) -> dict:
    key_of = jax.random.split(jax.random.key(seed), 4)
    near_null = draw_near_null(jax.random.fold_in(key_of[3], 71), 0)
    offsets = with_ends(jax.random.randint(key_of[1], (4,), 1, AGG), jax.random.fold_in(key_of[1], 1), 1, AGG - 1).astype(jnp.int32)
    owner_slot = jax.vmap(lambda own: jax.random.permutation(own, NAGG))(jax.random.split(key_of[2], N_TA * N_GZ * N_GY)).reshape((N_TA, N_GZ, N_GY, NAGG)).astype(jnp.int32)
    return {"near_null": near_null, "offsets": offsets, "owner_slot": owner_slot}


ridge_scale = 0.05
top_precision = lax.Precision.HIGHEST

def factor_pass(blocks):
    norm_count = blocks.shape[3] * blocks.shape[5]
    products = jnp.einsum('nkvcas,nkwcbs->nkavbw', blocks, blocks, precision=top_precision) / norm_count
    gram_real = products[:, :, 0, :, 0, :] + products[:, :, 1, :, 1, :]
    gram_imag = products[:, :, 0, :, 1, :] - products[:, :, 1, :, 0, :]
    width = gram_real.shape[-1]
    diag_mean = lax.optimization_barrier(jnp.mean(jnp.diagonal(gram_real, axis1=2, axis2=3), axis=-1))
    ridge_term = ridge_scale * (diag_mean + 1e-06)
    gram_real = jnp.moveaxis(gram_real, (2, 3), (0, 1))
    gram_imag = jnp.moveaxis(gram_imag, (2, 3), (0, 1))
    zero_batch = jnp.zeros_like(ridge_term)
    low_real = [[zero_batch] * width for row_idx in range(width)]
    low_imag = [[zero_batch] * width for row_idx in range(width)]
    for col_idx in range(width):
        remain = gram_real[col_idx, col_idx] + ridge_term
        for mid_idx in range(col_idx):
            remain = remain - low_real[col_idx][mid_idx] * low_real[col_idx][mid_idx]
            remain = remain - low_imag[col_idx][mid_idx] * low_imag[col_idx][mid_idx]
        diag_val = jnp.sqrt(remain)
        low_real[col_idx][col_idx] = diag_val
        for row_idx in range(col_idx + 1, width):
            sum_real = gram_real[row_idx, col_idx]
            sum_imag = gram_imag[row_idx, col_idx]
            for mid_idx in range(col_idx):
                left_real = low_real[row_idx][mid_idx]
                left_imag = low_imag[row_idx][mid_idx]
                right_real = low_real[col_idx][mid_idx]
                right_imag = low_imag[col_idx][mid_idx]
                sum_real = sum_real - (left_real * right_real + left_imag * right_imag)
                sum_imag = sum_imag - (left_imag * right_real - left_real * right_imag)
            low_real[row_idx][col_idx] = sum_real / diag_val
            low_imag[row_idx][col_idx] = sum_imag / diag_val
    inv_real = [[zero_batch] * width for row_idx in range(width)]
    inv_imag = [[zero_batch] * width for row_idx in range(width)]
    for col_idx in range(width):
        inv_real[col_idx][col_idx] = 1.0 / low_real[col_idx][col_idx]
        for row_idx in range(col_idx + 1, width):
            sum_real = zero_batch
            sum_imag = zero_batch
            for mid_idx in range(col_idx, row_idx):
                left_real = low_real[row_idx][mid_idx]
                left_imag = low_imag[row_idx][mid_idx]
                right_real = inv_real[mid_idx][col_idx]
                right_imag = inv_imag[mid_idx][col_idx]
                sum_real = sum_real + left_real * right_real - left_imag * right_imag
                sum_imag = sum_imag + left_real * right_imag + left_imag * right_real
            inv_real[row_idx][col_idx] = -sum_real / low_real[row_idx][row_idx]
            inv_imag[row_idx][col_idx] = -sum_imag / low_real[row_idx][row_idx]
    map_real = jnp.stack([jnp.stack([inv_real[w_idx][v_idx] for w_idx in range(width)], axis=-1) for v_idx in range(width)], axis=-2)
    map_imag = -jnp.stack([jnp.stack([inv_imag[w_idx][v_idx] for w_idx in range(width)], axis=-1) for v_idx in range(width)], axis=-2)
    mixing = jnp.stack([jnp.stack([map_real, map_imag], axis=3), jnp.stack([-map_imag, map_real], axis=3)], axis=2)
    return jnp.einsum('nkvcas,nkavbw->nkwcbs', blocks, mixing, precision=top_precision)

def two_passes(blocks):
    return factor_pass(factor_pass(blocks))

def reference(near_null, offsets, owner_slot):
    lattice = near_null.reshape(NT, NZ, NY, V, C, 2, NX)
    lattice = jnp.roll(lattice, -offsets[0], axis=0)
    lattice = jnp.roll(lattice, -offsets[1], axis=1)
    lattice = jnp.roll(lattice, -offsets[2], axis=2)
    lattice = jnp.roll(lattice, -offsets[3], axis=6)
    half_c = C // 2
    pieces = lattice.reshape(N_TA, AGG, N_GZ, AGG, N_GY, AGG, V, 2, half_c, 2, NAGG, AGG)
    pieces = pieces.transpose(0, 2, 4, 10, 7, 6, 8, 9, 1, 3, 5, 11)
    site_count = AGG * AGG * AGG * AGG
    device_count = N_TA * N_GZ * N_GY
    flattened = pieces.reshape(device_count * NAGG, 2, V, half_c, 2, site_count)
    source_of = jnp.argsort(owner_slot, axis=-1).astype(jnp.int32)
    device_base = (jnp.arange(device_count, dtype=jnp.int32) * NAGG).reshape(N_TA, N_GZ, N_GY, 1)
    packed = jnp.take(flattened, (device_base + source_of).reshape(-1), axis=0)
    per_peer = NAGG // N_TA
    packed = packed.reshape(N_TA, N_GZ, N_GY, N_TA, per_peer, 2, V, half_c, 2, site_count)
    owned_aggs = packed.transpose(3, 1, 2, 0, 4, 5, 6, 7, 8, 9).reshape(device_count, NAGG, 2, V, half_c, 2, site_count)
    result = lax.map(two_passes, owned_aggs)
    return result.reshape(device_count * NAGG, 2, V, half_c, 2, site_count)
```

```python
import functools

import jax
import jax.numpy as jnp
from jax import lax
from jax.experimental import pallas as pl
from jax.experimental.pallas import tpu as pltpu
from jax.sharding import PartitionSpec as P

MESH = pl.DeviceIdType.MESH

HIGH = lax.Precision.HIGHEST
RIDGE = 0.05


def swap_bits(arrays, bit, distance):
    lanes = lax.broadcasted_iota(jnp.int32, arrays[0].shape, 1)
    low = (lanes & distance) == 0
    out = list(arrays)
    for first in range(len(arrays)):
        if first & (1 << bit):
            continue
        second = first | (1 << bit)
        a, b = arrays[first], arrays[second]
        out[first] = jnp.where(low, a, pltpu.roll(b, distance, 1))
        out[second] = jnp.where(low, pltpu.roll(a, 128 - distance, 1), b)
    return out


def pack_kernel(off_ref, slot_ref, x_ref, s_ref, tiles, place):
    cell_z, cell_y = pl.program_id(0), pl.program_id(1)
    ot, oz, oy, ox = off_ref[0], off_ref[1], off_ref[2], off_ref[3]

    @pl.when((cell_z == 0) & (cell_y == 0))
    def _():
        def fill(i, _):
            place[i // 16, slot_ref[i // 16, i % 16]] = i % 16
            return 0
        lax.fori_loop(0, 128, fill, 0)

    lanes = lax.broadcasted_iota(jnp.int32, (12, 128), 1)
    inside = (lanes & 63) < 64 - ox
    for vb in range(3):
        arrays = []
        for t in range(4):
            for m in range(4):
                row = x_ref[(t + ot) & 3, 0, 0, 4 * vb + m]
                turned = pltpu.roll(row, 128 - ox, 1)
                arrays.append(jnp.where(inside, turned, pltpu.roll(turned, 64, 1)))
        for bit in range(4):
            arrays = swap_bits(arrays, bit, 4 << bit)
        for j in range(16):
            for part in range(3):
                tiles[j, 3 * vb + part] = arrays[j][4 * part:4 * part + 4]
    home = 2 * (cell_z >= 4 - oz).astype(jnp.int32) + (cell_y >= 4 - oy).astype(jnp.int32)
    lane3 = lax.broadcasted_iota(jnp.int32, (9, 4, 128), 2)
    mine = ((lane3 >> 4) & 3) < 4 - ot
    def emit(q, _):
        s_ref[q, 0, 0] = jnp.where(mine, tiles[place[home, q]], tiles[place[4 + home, q]])
        return 0
    lax.fori_loop(0, 16, emit, 0)


def pack(offsets, slots, x):
    def at(z, y, off, slot):
        return (0, (z + off[1]) & 3, (y + off[2]) & 3, 0, 0, 0)
    return pl.pallas_call(
        pack_kernel,
        out_shape=jax.ShapeDtypeStruct((16, 4, 4, 9, 4, 128), jnp.float32),
        grid_spec=pltpu.PrefetchScalarGridSpec(
            num_scalar_prefetch=2,
            grid=(4, 4),
            in_specs=[pl.BlockSpec((4, 1, 1, 12, 12, 128), at)],
            out_specs=pl.BlockSpec((16, 1, 1, 9, 4, 128), lambda z, y, off, slot: (0, z, y, 0, 0, 0)),
            scratch_shapes=[pltpu.VMEM((16, 9, 4, 128), jnp.float32), pltpu.SMEM((8, 16), jnp.int32)],
        ),
        compiler_params=pltpu.CompilerParams(dimension_semantics=("arbitrary", "arbitrary")),
        name="pack",
    )(offsets, slots, x)


def cmul_sub(ar, ai, br, bi, cr, ci):
    return ar - (br * cr - bi * ci), ai - (br * ci + bi * cr)


def factor(gr, gi, rows):
    gr, gi = list(gr), list(gi)
    diag = gr[0][0:1]
    for v in range(1, 12):
        diag = diag + gr[v][v:v + 1]
    ridge = RIDGE * (diag / 12.0 + 1e-06)
    low_r, low_i, inv = [None] * 12, [None] * 12, [None] * 12
    for j in range(12):
        d = jnp.sqrt(gr[j][j:j + 1] + ridge)
        inv[j] = 1.0 / d
        below = rows > j
        low_r[j] = jnp.where(below, gr[j] * inv[j], 0.0)
        low_i[j] = jnp.where(below, gi[j] * inv[j], 0.0)
        for w in range(j + 1, 12):
            wr, wi = low_r[j][w:w + 1], low_i[j][w:w + 1]
            gr[w] = gr[w] - (low_r[j] * wr + low_i[j] * wi)
            gi[w] = gi[w] - (low_i[j] * wr - low_r[j] * wi)
    xr, xi = [], []
    for c in range(12):
        ar = jnp.where(rows == c, inv[c], 0.0)
        ai = jnp.zeros_like(ar)
        for m in range(c, 12):
            if m > c:
                here = rows == m
                ar = jnp.where(here, ar * inv[m], ar)
                ai = jnp.where(here, ai * inv[m], ai)
            if m < 11:
                ar, ai = cmul_sub(ar, ai, low_r[m], low_i[m], ar[m:m + 1], ai[m:m + 1])
        xr.append(ar)
        xi.append(ai)
    return xr, xi


def small_product(ar, ai, entry, span):
    out_r, out_i = [], []
    for c in range(12):
        sr = si = None
        for l in span(c):
            er, ei = entry(l, c)
            tr = ar[l] * er - ai[l] * ei
            ti = ar[l] * ei + ai[l] * er
            sr, si = (tr, ti) if sr is None else (sr + tr, si + ti)
        out_r.append(sr)
        out_i.append(si)
    return out_r, out_i


def finish_kernel(off_ref, r_ref, o_ref, sites, grams, maps):
    ot = off_ref[0]
    lanes = lax.broadcasted_iota(jnp.int32, (12, 128), 1)
    mine = ((lanes >> 4) & 3) < 4 - ot

    def unpack(n, _):
        after = (n + 1) & 15
        for vb in range(3):
            arrays = []
            for cell in range(16):
                rows = pl.ds(cell * 36 + vb * 12, 12)
                arrays.append(jnp.where(mine, r_ref[n, rows], r_ref[after, rows]))
            for bit in range(4):
                arrays = swap_bits(arrays, bit, 4 << bit)
            arrays = swap_bits(arrays, 2, 64)
            for at in range(16):
                thi, ri, m = at >> 3, (at >> 2) & 1, at & 3
                sites[n, thi, pl.ds(ri * 12 + 4 * vb + m, 12, stride=24)] = arrays[at]
        return 0
    lax.fori_loop(0, 16, unpack, 0)

    def operand(group, c):
        parts = [sites[pl.ds(4 * group, 4), thi, pl.ds(c * 24, 24)].reshape(96, 128) for thi in range(2)]
        return jnp.concatenate(parts, axis=1)

    def gram(step, _):
        h, group = step // 4, step % 4
        def add(k, total):
            block = operand(group, h * 6 + k)
            return total + lax.dot_general(block, block, (((1,), (1,)), ((), ())), precision=HIGH, preferred_element_type=jnp.float32)
        total = lax.fori_loop(0, 6, add, jnp.zeros((96, 96), jnp.float32)) / 1536.0
        total = jnp.concatenate([total, jnp.zeros((96, 32), jnp.float32)], axis=1)
        for i in range(4):
            piece = total[24 * i:24 * i + 24]
            if i:
                piece = pltpu.roll(piece, 128 - 24 * i, 1)
            grams[pl.ds((h * 16 + group * 4 + i) * 24, 24)] = piece
        return 0
    lax.fori_loop(0, 8, gram, 0)

    lane128 = lax.broadcasted_iota(jnp.int32, (24, 128), 1)
    columns = []
    for four in range(6):
        stack = jnp.concatenate([grams[pl.ds(4 * four + i, 32, stride=24)] for i in range(4)], axis=0)
        turned = jnp.transpose(stack)[0:24]
        for i in range(4):
            columns.append(pltpu.roll(turned, 128 - 32 * i, 1) if i else turned)
    columns = [jnp.where(lane128 < 32, column, 0.0) for column in columns]
    rows = lax.broadcasted_iota(jnp.int32, (12, 128), 0)
    gr = [columns[w][0:12] + columns[12 + w][12:24] for w in range(12)]
    gi = [columns[12 + w][0:12] - columns[w][12:24] for w in range(12)]
    xr, xi = factor(gr, gi, rows)
    tr, ti = small_product(xr, xi, lambda l, c: (gr[c][l:l + 1], gi[c][l:l + 1]), lambda c: range(12))
    sr, si = small_product(tr, ti, lambda l, c: (xr[l][c:c + 1], -xi[l][c:c + 1]), lambda c: range(c + 1))
    yr, yi = factor(sr, si, rows)
    mr, mi = small_product(yr, yi, lambda l, c: (xr[c][l:l + 1], xi[c][l:l + 1]), lambda c: range(c, 12))

    for four in range(6):
        stack = None
        for i in range(4):
            r = 4 * four + i
            v = r % 12
            column = jnp.concatenate([mr[v], -mi[v]] if r < 12 else [mi[v], mr[v]], axis=0)
            column = jnp.where(lane128 < 32, column, 0.0)
            if i:
                column = pltpu.roll(column, 32 * i, 1)
            stack = column if stack is None else stack + column
        stack = jnp.concatenate([stack, jnp.zeros((104, 128), jnp.float32)], axis=0)
        turned = jnp.transpose(stack)
        for i in range(4):
            maps[pl.ds(4 * four + i, 32, stride=24)] = turned[32 * i:32 * i + 32]

    def apply(step, _):
        h, group = step // 4, step % 4
        parts = []
        for i in range(4):
            piece = maps[pl.ds((h * 16 + group * 4 + i) * 24, 24)]
            parts.append(pltpu.roll(piece, 24 * i, 1) if i else piece)
        parts.append(jnp.zeros((32, 128), jnp.float32))
        mixing = jnp.transpose(jnp.concatenate(parts, axis=0))[0:96, 0:96]
        def one(k, _):
            block = operand(group, h * 6 + k)
            out = lax.dot_general(mixing, block, (((1,), (0,)), ((), ())), precision=HIGH, preferred_element_type=jnp.float32)
            for i in range(4):
                for ri in range(2):
                    for col in range(2):
                        start = (((group * 4 + i) * 2 + h) * 12) * 24 + k * 4 + col * 2 + ri
                        o_ref[pl.ds(start, 12, stride=24)] = out[24 * i + 12 * ri:24 * i + 12 * ri + 12, 128 * col:128 * col + 128]
            return 0
        lax.fori_loop(0, 6, one, 0)
        return 0
    lax.fori_loop(0, 8, apply, 0)


def finish(offsets, r):
    out = pl.pallas_call(
        finish_kernel,
        out_shape=jax.ShapeDtypeStruct((9216, 128), jnp.float32),
        in_specs=[pl.BlockSpec(memory_space=pltpu.SMEM), pl.BlockSpec(memory_space=pltpu.VMEM)],
        out_specs=pl.BlockSpec(memory_space=pltpu.VMEM),
        scratch_shapes=[
            pltpu.VMEM((16, 2, 288, 128), jnp.float32),
            pltpu.VMEM((768, 128), jnp.float32),
            pltpu.VMEM((768, 128), jnp.float32),
        ],
        name="finish",
    )(offsets, r.reshape(16, 576, 128))
    out = out.reshape(16, 2, 12, 6, 2, 2, 128)
    return out.transpose(0, 1, 2, 3, 5, 4, 6).reshape(16, 2, 12, 6, 2, 256)


WAYS = ((1, 1), (1, 0), (0, 1), (0, 0))


def exchange_kernel(oz, oy, s_ref, r_ref, send, recv, local):
    a, b, c = lax.axis_index("ta"), lax.axis_index("gz"), lax.axis_index("gy")
    n_a, n_b, n_c = lax.axis_size("ta"), lax.axis_size("gz"), lax.axis_size("gy")
    spans_z = ((0, 4 - oz), (4 - oz, oz))
    spans_y = ((0, 4 - oy), (4 - oy, oy))

    barrier = pltpu.get_barrier_semaphore()

    def greet(step, _):
        q = lax.rem(a + step, n_a)
        for dz, dy in WAYS[:3]:
            peer = (q, lax.rem(b + dz, n_b), lax.rem(c + dy, n_c))
            pl.semaphore_signal(barrier, inc=1, device_id=peer, device_id_type=MESH)

        @pl.when(step < n_a)
        def _():
            pl.semaphore_signal(barrier, inc=1, device_id=(q, b, c), device_id_type=MESH)

        return 0

    lax.fori_loop(1, n_a + 1, greet, 0)
    pl.semaphore_wait(barrier, 4 * n_a - 1)

    def view(ref, at, dz, dy):
        z0, nz = spans_z[dz]
        y0, ny = spans_y[dy]
        return ref.at[at, pl.ds(z0, nz), pl.ds(y0, ny)]

    def copy(way, q, lands):
        dz, dy = WAYS[way]
        return pltpu.make_async_remote_copy(
            view(s_ref, q, dz, dy),
            view(r_ref, lands, dz, dy),
            send.at[way, q],
            recv.at[way, lands],
            device_id=(q, lax.rem(b + n_b - dz, n_b), lax.rem(c + n_c - dy, n_c)),
            device_id_type=MESH,
        )

    def start(step, _):
        q = lax.rem(a + step, n_a)
        for way in range(3):
            copy(way, q, a).start()
        pl.when(step < n_a)(copy(3, q, a).start)
        return 0

    own = pltpu.make_async_copy(view(s_ref, a, 0, 0), view(r_ref, a, 0, 0), local)
    lax.fori_loop(1, n_a + 1, start, 0)
    own.start()

    def finish_one(way, q):
        one = copy(way, q, q)
        one.wait_send()
        one.wait_recv()

    def wait(step, _):
        q = lax.rem(a + step, n_a)
        for way in range(3):
            finish_one(way, q)
        pl.when(step < n_a)(functools.partial(finish_one, 3, q))
        return 0

    lax.fori_loop(1, n_a + 1, wait, 0)
    own.wait()


def exchange(s, oz, oy):
    return pl.pallas_call(
        functools.partial(exchange_kernel, oz, oy),
        out_shape=jax.ShapeDtypeStruct(s.shape, s.dtype),
        in_specs=[pl.BlockSpec(memory_space=pl.ANY)],
        out_specs=pl.BlockSpec(memory_space=pl.ANY),
        scratch_shapes=[pltpu.SemaphoreType.DMA((4, 16)), pltpu.SemaphoreType.DMA((4, 16)), pltpu.SemaphoreType.DMA],
        compiler_params=pltpu.CompilerParams(has_side_effects=True, collective_id=3 * (oz - 1) + oy - 1),
        name=f"exchange_{oz}{oy}",
    )(s)


def ahead(array, axis):
    length = lax.axis_size(axis)
    return lax.ppermute(array, axis, [(i, (i + 1) % length) for i in range(length)])


def per_device(near_null, offsets, owner_slot):
    slots = owner_slot.reshape(1, 16)
    for axis in ("gy", "gz", "ta"):
        slots = jnp.concatenate([slots, ahead(slots, axis)], axis=0)
    s = pack(offsets, slots, near_null)
    branches = [functools.partial(exchange, oz=oz, oy=oy) for oz in (1, 2, 3) for oy in (1, 2, 3)]
    r = lax.switch(3 * (offsets[1] - 1) + offsets[2] - 1, branches, s)
    return finish(offsets, r)


def solution(mesh):
    return jax.shard_map(
        per_device,
        mesh=mesh,
        in_specs=(P("ta", "gz", "gy", None, None, None), P(), P("ta", "gz", "gy", None)),
        out_specs=P(("ta", "gz", "gy"), None, None, None, None, None),
        check_vma=False,
    )
```

```python
import functools

import jax
import jax.numpy as jnp
from jax import lax
from jax.experimental import pallas as pl
from jax.experimental.pallas import tpu as pltpu
from jax.sharding import PartitionSpec as P

MESH = pl.DeviceIdType.MESH

HIGH = lax.Precision.HIGHEST
RIDGE = 0.05


def swap_bits(arrays, bit, distance):
    lanes = lax.broadcasted_iota(jnp.int32, arrays[0].shape, 1)
    low = (lanes & distance) == 0
    out = list(arrays)
    for first in range(len(arrays)):
        if first & (1 << bit):
            continue
        second = first | (1 << bit)
        a, b = arrays[first], arrays[second]
        out[first] = jnp.where(low, a, pltpu.roll(b, distance, 1))
        out[second] = jnp.where(low, pltpu.roll(a, 128 - distance, 1), b)
    return out


def cmul_sub(ar, ai, br, bi, cr, ci):
    return ar - (br * cr - bi * ci), ai - (br * ci + bi * cr)


def factor(gr, gi, rows):
    gr, gi = list(gr), list(gi)
    diag = gr[0][0:1]
    for v in range(1, 12):
        diag = diag + gr[v][v:v + 1]
    ridge = RIDGE * (diag / 12.0 + 1e-06)
    low_r, low_i, inv = [None] * 12, [None] * 12, [None] * 12
    for j in range(12):
        d = jnp.sqrt(gr[j][j:j + 1] + ridge)
        inv[j] = 1.0 / d
        below = rows > j
        low_r[j] = jnp.where(below, gr[j] * inv[j], 0.0)
        low_i[j] = jnp.where(below, gi[j] * inv[j], 0.0)
        for w in range(j + 1, 12):
            wr, wi = low_r[j][w:w + 1], low_i[j][w:w + 1]
            gr[w] = gr[w] - (low_r[j] * wr + low_i[j] * wi)
            gi[w] = gi[w] - (low_i[j] * wr - low_r[j] * wi)
    xr, xi = [], []
    for c in range(12):
        ar = jnp.where(rows == c, inv[c], 0.0)
        ai = jnp.zeros_like(ar)
        for m in range(c, 12):
            if m > c:
                here = rows == m
                ar = jnp.where(here, ar * inv[m], ar)
                ai = jnp.where(here, ai * inv[m], ai)
            if m < 11:
                ar, ai = cmul_sub(ar, ai, low_r[m], low_i[m], ar[m:m + 1], ai[m:m + 1])
        xr.append(ar)
        xi.append(ai)
    return xr, xi


def small_product(ar, ai, entry, span):
    out_r, out_i = [], []
    for c in range(12):
        sr = si = None
        for l in span(c):
            er, ei = entry(l, c)
            tr = ar[l] * er - ai[l] * ei
            ti = ar[l] * ei + ai[l] * er
            sr, si = (tr, ti) if sr is None else (sr + tr, si + ti)
        out_r.append(sr)
        out_i.append(si)
    return out_r, out_i


def finish_kernel(off_ref, r_ref, o_ref, sites, grams, maps):
    ot = off_ref[0]
    lanes = lax.broadcasted_iota(jnp.int32, (12, 128), 1)
    mine = ((lanes >> 4) & 3) < 4 - ot
    turn = (lanes & 124) | ((lanes + off_ref[3]) & 3)

    def unpack(n, _):
        after = (n + 1) & 15
        for vb in range(3):
            arrays = []
            for cell in range(16):
                rows = pl.ds(cell * 36 + vb * 12, 12)
                arrays.append(jnp.where(mine, r_ref[n, rows], r_ref[after, rows]))
            for bit in range(4):
                arrays = swap_bits(arrays, bit, 4 << bit)
            arrays = swap_bits(arrays, 2, 64)
            arrays = [jnp.take_along_axis(array, turn, axis=1, mode="promise_in_bounds") for array in arrays]
            for at in range(16):
                thi, ri, m = at >> 3, (at >> 2) & 1, at & 3
                sites[n, thi, pl.ds(ri * 12 + 4 * vb + m, 12, stride=24)] = arrays[at]
        return 0
    lax.fori_loop(0, 16, unpack, 0)

    def operand(group, c):
        parts = [sites[pl.ds(4 * group, 4), thi, pl.ds(c * 24, 24)].reshape(96, 128) for thi in range(2)]
        return jnp.concatenate(parts, axis=1)

    def gram(step, _):
        h, group = step // 4, step % 4
        def add(k, total):
            block = operand(group, h * 6 + k)
            return total + lax.dot_general(block, block, (((1,), (1,)), ((), ())), precision=HIGH, preferred_element_type=jnp.float32)
        total = lax.fori_loop(0, 6, add, jnp.zeros((96, 96), jnp.float32)) / 1536.0
        total = jnp.concatenate([total, jnp.zeros((96, 32), jnp.float32)], axis=1)
        for i in range(4):
            piece = total[24 * i:24 * i + 24]
            if i:
                piece = pltpu.roll(piece, 128 - 24 * i, 1)
            grams[pl.ds((h * 16 + group * 4 + i) * 24, 24)] = piece
        return 0
    lax.fori_loop(0, 8, gram, 0)

    lane128 = lax.broadcasted_iota(jnp.int32, (24, 128), 1)
    columns = []
    for four in range(6):
        stack = jnp.concatenate([grams[pl.ds(4 * four + i, 32, stride=24)] for i in range(4)], axis=0)
        turned = jnp.transpose(stack)[0:24]
        for i in range(4):
            columns.append(pltpu.roll(turned, 128 - 32 * i, 1) if i else turned)
    columns = [jnp.where(lane128 < 32, column, 0.0) for column in columns]
    rows = lax.broadcasted_iota(jnp.int32, (12, 128), 0)
    gr = [columns[w][0:12] + columns[12 + w][12:24] for w in range(12)]
    gi = [columns[12 + w][0:12] - columns[w][12:24] for w in range(12)]
    xr, xi = factor(gr, gi, rows)
    tr, ti = small_product(xr, xi, lambda l, c: (gr[c][l:l + 1], gi[c][l:l + 1]), lambda c: range(12))
    sr, si = small_product(tr, ti, lambda l, c: (xr[l][c:c + 1], -xi[l][c:c + 1]), lambda c: range(c + 1))
    yr, yi = factor(sr, si, rows)
    mr, mi = small_product(yr, yi, lambda l, c: (xr[c][l:l + 1], xi[c][l:l + 1]), lambda c: range(c, 12))

    for four in range(6):
        stack = None
        for i in range(4):
            r = 4 * four + i
            v = r % 12
            column = jnp.concatenate([mr[v], -mi[v]] if r < 12 else [mi[v], mr[v]], axis=0)
            column = jnp.where(lane128 < 32, column, 0.0)
            if i:
                column = pltpu.roll(column, 32 * i, 1)
            stack = column if stack is None else stack + column
        stack = jnp.concatenate([stack, jnp.zeros((104, 128), jnp.float32)], axis=0)
        turned = jnp.transpose(stack)
        for i in range(4):
            maps[pl.ds(4 * four + i, 32, stride=24)] = turned[32 * i:32 * i + 32]

    def apply(step, _):
        h, group = step // 4, step % 4
        parts = []
        for i in range(4):
            piece = maps[pl.ds((h * 16 + group * 4 + i) * 24, 24)]
            parts.append(pltpu.roll(piece, 24 * i, 1) if i else piece)
        parts.append(jnp.zeros((32, 128), jnp.float32))
        mixing = jnp.transpose(jnp.concatenate(parts, axis=0))[0:96, 0:96]
        def one(k, _):
            block = operand(group, h * 6 + k)
            out = lax.dot_general(mixing, block, (((1,), (0,)), ((), ())), precision=HIGH, preferred_element_type=jnp.float32)
            for i in range(4):
                for ri in range(2):
                    for col in range(2):
                        start = (((group * 4 + i) * 2 + h) * 12) * 24 + k * 4 + col * 2 + ri
                        o_ref[pl.ds(start, 12, stride=24)] = out[24 * i + 12 * ri:24 * i + 12 * ri + 12, 128 * col:128 * col + 128]
            return 0
        lax.fori_loop(0, 6, one, 0)
        return 0
    lax.fori_loop(0, 8, apply, 0)


def finish(offsets, r):
    out = pl.pallas_call(
        finish_kernel,
        out_shape=jax.ShapeDtypeStruct((9216, 128), jnp.float32),
        in_specs=[pl.BlockSpec(memory_space=pltpu.SMEM), pl.BlockSpec(memory_space=pltpu.VMEM)],
        out_specs=pl.BlockSpec(memory_space=pltpu.VMEM),
        scratch_shapes=[
            pltpu.VMEM((16, 2, 288, 128), jnp.float32),
            pltpu.VMEM((768, 128), jnp.float32),
            pltpu.VMEM((768, 128), jnp.float32),
        ],
        name="finish",
    )(offsets, r.reshape(16, 576, 128))
    out = out.reshape(16, 2, 12, 6, 2, 2, 128)
    return out.transpose(0, 1, 2, 3, 5, 4, 6).reshape(16, 2, 12, 6, 2, 256)


def exchange_kernel(oz, oy, off_ref, place_ref, x_ref, r_ref, tiles, s_ref, send, recv, local):
    a, b, c = lax.axis_index("ta"), lax.axis_index("gz"), lax.axis_index("gy")
    n_a, n_b, n_c = lax.axis_size("ta"), lax.axis_size("gz"), lax.axis_size("gy")
    ot, ox = off_ref[0], off_ref[3]
    spans = ((0, 4 - oy), (4 - oy, oy))

    barrier = pltpu.get_barrier_semaphore()

    def greet(step, _):
        q = lax.rem(a + step, n_a)
        for dz, dy in ((1, 1), (1, 0), (0, 1)):
            peer = (q, lax.rem(b + dz, n_b), lax.rem(c + dy, n_c))
            pl.semaphore_signal(barrier, inc=1, device_id=peer, device_id_type=MESH)

        @pl.when(step < n_a)
        def _():
            pl.semaphore_signal(barrier, inc=1, device_id=(q, b, c), device_id_type=MESH)

        return 0

    lax.fori_loop(1, n_a + 1, greet, 0)

    lanes = lax.broadcasted_iota(jnp.int32, (8, 128), 1)
    stays = (lanes & 3) >= ox
    lanes4 = lax.broadcasted_iota(jnp.int32, (4, 128), 1)
    mine = ((lanes4 >> 4) & 3) < 4 - ot

    def copy(z, dz, dy, q, lands):
        y0, ny = spans[dy]
        return pltpu.make_async_remote_copy(
            s_ref.at[q, z, pl.ds(y0, ny)],
            r_ref.at[lands, z, pl.ds(y0, ny)],
            send.at[z, dy, q],
            recv.at[z, dy, lands],
            device_id=(q, lax.rem(b + n_b - dz, n_b), lax.rem(c + n_c - dy, n_c)),
            device_id_type=MESH,
        )

    def own(z):
        y0, ny = spans[0]
        return pltpu.make_async_copy(s_ref.at[a, z, pl.ds(y0, ny)], r_ref.at[a, z, pl.ds(y0, ny)], local.at[z])

    def plane(z, dz):
        from_z = lax.rem(z + oz, 4)

        def spread(step, _):
            vb, part = step // 6, lax.rem(step, 6)
            rows = pl.ds(pl.multiple_of(8 * part, 8), 8)
            arrays = [x_ref[(t + ot) & 3, from_z, 4 * vb + m, rows] for t in range(4) for m in range(4)]
            for bit in range(4):
                arrays = swap_bits(arrays, bit, 4 << bit)
            for j in range(16):
                row = pl.multiple_of(j * 144 + vb * 48 + 8 * part, 8)
                tiles[pl.ds(row, 8)] = jnp.where(stays, arrays[j], arrays[(j + 1) % 16])
            return 0

        lax.fori_loop(0, 18, spread, 0)

        def emit(q, _):
            for y in range(4):
                home = 2 * dz + (y >= 4 - oy)
                first = place_ref[home, q] * 144 + (y + oy) % 4
                second = place_ref[4 + home, q] * 144 + (y + oy) % 4
                for g in range(9):
                    s_ref[q, z, y, g] = jnp.where(
                        mine,
                        tiles[pl.ds(first + 16 * g, 4, stride=4)],
                        tiles[pl.ds(second + 16 * g, 4, stride=4)],
                    )
            return 0

        lax.fori_loop(0, 16, emit, 0)

    def start(z, dz):
        def one(step, _):
            q = lax.rem(a + step, n_a)
            copy(z, dz, 1, q, a).start()
            if dz:
                copy(z, dz, 0, q, a).start()
            else:
                pl.when(step < n_a)(copy(z, dz, 0, q, a).start)
            return 0

        lax.fori_loop(1, n_a + 1, one, 0)
        if not dz:
            own(z).start()

    def finish_one(z, dz, dy, q):
        one = copy(z, dz, dy, q, q)
        one.wait_send()
        one.wait_recv()

    def wait(z, dz):
        def one(step, _):
            q = lax.rem(a + step, n_a)
            finish_one(z, dz, 1, q)
            if dz:
                finish_one(z, dz, 0, q)
            else:
                pl.when(step < n_a)(functools.partial(finish_one, z, dz, 0, q))
            return 0

        lax.fori_loop(1, n_a + 1, one, 0)
        if not dz:
            own(z).wait()

    def both(dz, first, last):
        def run(z, _):
            plane(z, dz)

            @pl.when(z == ORDER_FIRST[oz])
            def _():
                pl.semaphore_wait(barrier, 4 * n_a - 1)

            start(z, dz)
            return 0

        lax.fori_loop(first, last, run, 0)

    both(1, 4 - oz, 4)
    both(0, 0, 4 - oz)

    for dz, first, last in ((1, 4 - oz, 4), (0, 0, 4 - oz)):
        def done(z, _):
            wait(z, dz)
            return 0

        lax.fori_loop(first, last, done, 0)


ORDER_FIRST = {1: 3, 2: 2, 3: 1}


def exchange(offsets, place, x, oz, oy):
    return pl.pallas_call(
        functools.partial(exchange_kernel, oz, oy),
        out_shape=jax.ShapeDtypeStruct((16, 4, 4, 9, 4, 128), jnp.float32),
        in_specs=[
            pl.BlockSpec(memory_space=pltpu.SMEM),
            pl.BlockSpec(memory_space=pltpu.SMEM),
            pl.BlockSpec(memory_space=pltpu.VMEM),
        ],
        out_specs=pl.BlockSpec(memory_space=pl.ANY),
        scratch_shapes=[
            pltpu.VMEM((16 * 144, 128), jnp.float32),
            pltpu.VMEM((16, 4, 4, 9, 4, 128), jnp.float32),
            pltpu.SemaphoreType.DMA((4, 2, 16)),
            pltpu.SemaphoreType.DMA((4, 2, 16)),
            pltpu.SemaphoreType.DMA((4,)),
        ],
        compiler_params=pltpu.CompilerParams(has_side_effects=True, collective_id=3 * (oz - 1) + oy - 1),
        name=f"exchange_{oz}{oy}",
    )(offsets, place, x)


def slots_of_homes(slots):
    names = ("ta", "gz", "gy")
    sizes = [lax.axis_size(name) for name in names]
    ranks = [(i, j, k) for i in range(sizes[0]) for j in range(sizes[1]) for k in range(sizes[2])]
    number = {rank: n for n, rank in enumerate(ranks)}
    rows = [slots]
    for code in range(1, 8):
        by = ((code >> 2) & 1, (code >> 1) & 1, code & 1)
        pairs = [(n, number[tuple((r + d) % size for r, d, size in zip(rank, by, sizes))]) for n, rank in enumerate(ranks)]
        rows.append(lax.ppermute(slots, names, pairs))
    return jnp.concatenate(rows, axis=0)


def per_device(near_null, offsets, owner_slot):
    slots = slots_of_homes(owner_slot.reshape(1, 16))
    spots = jnp.arange(16, dtype=jnp.int32)
    hits = slots[:, :, None] == spots[None, None, :]
    place = jnp.sum(jnp.where(hits, spots[None, :, None], 0), axis=1)
    x = near_null.transpose(0, 1, 3, 4, 2, 5).reshape(4, 4, 12, 48, 128)
    branches = [functools.partial(exchange, oz=oz, oy=oy) for oz in (1, 2, 3) for oy in (1, 2, 3)]
    r = lax.switch(3 * (offsets[1] - 1) + offsets[2] - 1, branches, offsets, place, x)
    return finish(offsets, r)


def solution(mesh):
    return jax.shard_map(
        per_device,
        mesh=mesh,
        in_specs=(P("ta", "gz", "gy", None, None, None), P(), P("ta", "gz", "gy", None)),
        out_specs=P(("ta", "gz", "gy"), None, None, None, None, None),
        check_vma=False,
    )
```

```python
import functools

import jax
import jax.numpy as jnp
from jax import lax
from jax.experimental import pallas as pl
from jax.experimental.pallas import tpu as pltpu
from jax.sharding import PartitionSpec as P

MESH = pl.DeviceIdType.MESH

HIGH = lax.Precision.HIGHEST
RIDGE = 0.05


def swap_bits(arrays, bit, distance):
    lanes = lax.broadcasted_iota(jnp.int32, arrays[0].shape, 1)
    low = (lanes & distance) == 0
    out = list(arrays)
    for first in range(len(arrays)):
        if first & (1 << bit):
            continue
        second = first | (1 << bit)
        a, b = arrays[first], arrays[second]
        out[first] = jnp.where(low, a, pltpu.roll(b, distance, 1))
        out[second] = jnp.where(low, pltpu.roll(a, 128 - distance, 1), b)
    return out


def cmul_sub(ar, ai, br, bi, cr, ci):
    return ar - (br * cr - bi * ci), ai - (br * ci + bi * cr)


def factor(gr, gi, rows):
    gr, gi = list(gr), list(gi)
    diag = gr[0][0:1]
    for v in range(1, 12):
        diag = diag + gr[v][v:v + 1]
    ridge = RIDGE * (diag / 12.0 + 1e-06)
    low_r, low_i, inv = [None] * 12, [None] * 12, [None] * 12
    for j in range(12):
        d = jnp.sqrt(gr[j][j:j + 1] + ridge)
        inv[j] = 1.0 / d
        below = rows > j
        low_r[j] = jnp.where(below, gr[j] * inv[j], 0.0)
        low_i[j] = jnp.where(below, gi[j] * inv[j], 0.0)
        for w in range(j + 1, 12):
            wr, wi = low_r[j][w:w + 1], low_i[j][w:w + 1]
            gr[w] = gr[w] - (low_r[j] * wr + low_i[j] * wi)
            gi[w] = gi[w] - (low_i[j] * wr - low_r[j] * wi)
    xr, xi = [], []
    for c in range(12):
        ar = jnp.where(rows == c, inv[c], 0.0)
        ai = jnp.zeros_like(ar)
        for m in range(c, 12):
            if m > c:
                here = rows == m
                ar = jnp.where(here, ar * inv[m], ar)
                ai = jnp.where(here, ai * inv[m], ai)
            if m < 11:
                ar, ai = cmul_sub(ar, ai, low_r[m], low_i[m], ar[m:m + 1], ai[m:m + 1])
        xr.append(ar)
        xi.append(ai)
    return xr, xi


def small_product(ar, ai, entry, span):
    out_r, out_i = [], []
    for c in range(12):
        sr = si = None
        for l in span(c):
            er, ei = entry(l, c)
            tr = ar[l] * er - ai[l] * ei
            ti = ar[l] * ei + ai[l] * er
            sr, si = (tr, ti) if sr is None else (sr + tr, si + ti)
        out_r.append(sr)
        out_i.append(si)
    return out_r, out_i


def split(x):
    first = x.astype(jnp.bfloat16)
    rest = x - first.astype(jnp.float32)
    second = rest.astype(jnp.bfloat16)
    return first, second, (rest - second.astype(jnp.float32)).astype(jnp.bfloat16)


def product(left, right, at):
    return lax.dot_general(left, right, (((1,), (at,)), ((), ())), preferred_element_type=jnp.float32)


def operand(ref, first, c):
    rows = pl.ds(pl.multiple_of(c * 24, 8), 24)
    parts = [ref[pl.ds(first, 4), thi, rows].reshape(96, 128) for thi in range(2)]
    return jnp.concatenate(parts, axis=1)


def finish_kernel(gram_ref, sites_ref, o_ref, maps):
    step = pl.program_id(0)
    lane128 = lax.broadcasted_iota(jnp.int32, (24, 128), 1)

    @pl.when(step == 0)
    def _():
        columns = []
        for four in range(6):
            stack = jnp.concatenate([gram_ref[pl.ds(4 * four + i, 32, stride=24)] for i in range(4)], axis=0)
            turned = jnp.transpose(stack)[0:24]
            for i in range(4):
                columns.append(pltpu.roll(turned, 128 - 32 * i, 1) if i else turned)
        columns = [jnp.where(lane128 < 32, column, 0.0) for column in columns]
        rows = lax.broadcasted_iota(jnp.int32, (12, 128), 0)
        gr = [columns[w][0:12] + columns[12 + w][12:24] for w in range(12)]
        gi = [columns[12 + w][0:12] - columns[w][12:24] for w in range(12)]
        xr, xi = factor(gr, gi, rows)
        tr, ti = small_product(xr, xi, lambda l, c: (gr[c][l:l + 1], gi[c][l:l + 1]), lambda c: range(12))
        sr, si = small_product(tr, ti, lambda l, c: (xr[l][c:c + 1], -xi[l][c:c + 1]), lambda c: range(c + 1))
        yr, yi = factor(sr, si, rows)
        mr, mi = small_product(yr, yi, lambda l, c: (xr[c][l:l + 1], xi[c][l:l + 1]), lambda c: range(c, 12))
        for four in range(6):
            stack = None
            for i in range(4):
                r = 4 * four + i
                v = r % 12
                column = jnp.concatenate([mr[v], -mi[v]] if r < 12 else [mi[v], mr[v]], axis=0)
                column = jnp.where(lane128 < 32, column, 0.0)
                if i:
                    column = pltpu.roll(column, 32 * i, 1)
                stack = column if stack is None else stack + column
            stack = jnp.concatenate([stack, jnp.zeros((104, 128), jnp.float32)], axis=0)
            turned = jnp.transpose(stack)
            for i in range(4):
                maps[pl.ds(4 * four + i, 32, stride=24)] = turned[32 * i:32 * i + 32]

    for h in range(2):
        parts = []
        for i in range(4):
            piece = maps[pl.ds(pl.multiple_of((h * 16 + 4 * step + i) * 24, 8), 24)]
            parts.append(pltpu.roll(piece, 24 * i, 1) if i else piece)
        parts.append(jnp.zeros((32, 128), jnp.float32))
        mixing = jnp.transpose(jnp.concatenate(parts, axis=0))[0:96]
        a1, a2, a3 = split(mixing)
        left = jnp.concatenate([a1, a2], axis=1)
        right = jnp.concatenate([a1, a3], axis=1)
        still = jnp.zeros((32, 256), jnp.bfloat16)

        def one(k, _):
            b1, b2, b3 = split(operand(sites_ref, 0, h * 6 + k))
            b1, b2, b3 = [jnp.concatenate([b, still], axis=0) for b in (b1, b2, b3)]
            out = product(right, jnp.concatenate([b3, b1], axis=0), 0)
            out = out + product(left, jnp.concatenate([b2, b2], axis=0), 0)
            out = out + product(left, jnp.concatenate([b1, b1], axis=0), 0)
            for i in range(4):
                for ri in range(2):
                    for col in range(2):
                        start = ((i * 2 + h) * 12) * 24 + k * 4 + col * 2 + ri
                        o_ref[pl.ds(start, 12, stride=24)] = out[24 * i + 12 * ri:24 * i + 12 * ri + 12, 128 * col:128 * col + 128]
            return 0

        lax.fori_loop(0, 6, one, 0)


def finish(grams, sites):
    out = pl.pallas_call(
        finish_kernel,
        out_shape=jax.ShapeDtypeStruct((9216, 128), jnp.float32),
        grid=(4,),
        in_specs=[
            pl.BlockSpec((768, 128), lambda i: (0, 0)),
            pl.BlockSpec((4, 2, 288, 128), lambda i: (i, 0, 0, 0)),
        ],
        out_specs=pl.BlockSpec((2304, 128), lambda i: (i, 0)),
        scratch_shapes=[pltpu.VMEM((768, 128), jnp.float32)],
        compiler_params=pltpu.CompilerParams(dimension_semantics=("arbitrary",)),
        name="finish",
    )(grams, sites)
    out = out.reshape(16, 2, 12, 6, 2, 2, 128)
    return out.transpose(0, 1, 2, 3, 5, 4, 6).reshape(16, 2, 12, 6, 2, 256)


def exchange_kernel(oz, oy, off_ref, row_ref, x_ref, out_ref, gram_ref, place, rows_ref, tiles, s_ref, r_ref, sites, send, recv, row_send, row_recv, local):
    a, b, c = lax.axis_index("ta"), lax.axis_index("gz"), lax.axis_index("gy")
    n_a, n_b, n_c = lax.axis_size("ta"), lax.axis_size("gz"), lax.axis_size("gy")
    ot, ox = off_ref[0], off_ref[3]
    spans = ((0, 4 - oy), (4 - oy, oy))
    groups = ((3, 1, 1),) + {1: ((0, 3, 0),), 2: ((2, 1, 1), (0, 2, 0)), 3: ((1, 2, 1), (0, 1, 0))}[oz]

    def peer(code, sign):
        da, db, dc = (code >> 2) & 1, (code >> 1) & 1, code & 1
        return (lax.rem(a + n_a + sign * da, n_a), lax.rem(b + n_b + sign * db, n_b), lax.rem(c + n_c + sign * dc, n_c))

    barrier = pltpu.get_barrier_semaphore()

    def greet(step, _):
        q = lax.rem(a + step, n_a)
        for code in (3, 2, 1):
            device = (q,) + peer(code, 1)[1:]
            pl.semaphore_signal(barrier, inc=1, device_id=device, device_id_type=MESH)

        @pl.when(step > 0)
        def _():
            pl.semaphore_signal(barrier, inc=1, device_id=(q, b, c), device_id_type=MESH)

        return 0

    for code in (1, 2, 3, 5, 6, 7):
        pl.semaphore_signal(barrier, inc=1, device_id=peer(code, -1), device_id_type=MESH)
    lax.fori_loop(0, n_a, greet, 0)
    pl.semaphore_wait(barrier, 4 * n_a + 5)

    def row_copy(code):
        return pltpu.make_async_remote_copy(
            row_ref,
            rows_ref.at[code],
            row_send.at[code],
            row_recv.at[code],
            device_id=peer(code, 1),
            device_id_type=MESH,
        )

    own_row = pltpu.make_async_copy(row_ref, rows_ref.at[0], local.at[0])
    own_row.start()
    for code in range(1, 8):
        row_copy(code).start()

    lanes = lax.broadcasted_iota(jnp.int32, (8, 128), 1)
    stays = (lanes & 3) >= ox
    turn = (lanes & 124) | ((lanes + ox) & 3)
    mine = ((lanes >> 4) & 3) < 4 - ot
    mine4 = ((lax.broadcasted_iota(jnp.int32, (4, 128), 1) >> 4) & 3) < 4 - ot

    def copy(group, dy, q, lands):
        z0, nz, dz = groups[group]
        y0, ny = spans[dy]
        return pltpu.make_async_remote_copy(
            s_ref.at[q, pl.ds(z0, nz), pl.ds(y0, ny)],
            r_ref.at[lands, pl.ds(z0, nz), pl.ds(y0, ny)],
            send.at[group, dy, q],
            recv.at[group, dy, lands],
            device_id=(q, lax.rem(b + n_b - dz, n_b), lax.rem(c + n_c - dy, n_c)),
            device_id_type=MESH,
        )

    last = len(groups) - 1
    z_own, nz_own, _ = groups[last]
    own = pltpu.make_async_copy(
        s_ref.at[a, pl.ds(z_own, nz_own), pl.ds(0, 4 - oy)],
        r_ref.at[a, pl.ds(z_own, nz_own), pl.ds(0, 4 - oy)],
        local.at[1],
    )

    def spread_plane(z):
        from_z = lax.rem(z + oz, 4)

        def spread(step, _):
            vb, part = step // 6, lax.rem(step, 6)
            rows = pl.ds(pl.multiple_of(8 * part, 8), 8)
            arrays = [x_ref[(t + ot) & 3, from_z, 4 * vb + m, rows] for t in range(4) for m in range(4)]
            for bit in range(4):
                arrays = swap_bits(arrays, bit, 4 << bit)
            for j in range(16):
                row = pl.multiple_of(j * 144 + vb * 48 + 8 * part, 8)
                tiles[pl.ds(row, 8)] = jnp.where(stays, arrays[j], arrays[(j + 1) % 16])
            return 0

        lax.fori_loop(0, 18, spread, 0)

    def emit_plane(z):
        dz = (z + oz) // 4

        def emit(q, _):
            for y in range(4):
                home = 2 * dz + (y + oy) // 4
                first = place[home, 0, q] * 144 + (y + oy) % 4
                second = place[4 + home, 0, q] * 144 + (y + oy) % 4
                for g in range(9):
                    s_ref[q, z, y, g] = jnp.where(
                        mine4,
                        tiles[pl.ds(first + 16 * g, 4, stride=4)],
                        tiles[pl.ds(second + 16 * g, 4, stride=4)],
                    )
            return 0

        lax.fori_loop(0, 16, emit, 0)

    def begin(group, q, step):
        copy(group, 1, q, a).start()
        if groups[group][2]:
            copy(group, 0, q, a).start()
        else:
            pl.when(step > 0)(copy(group, 0, q, a).start)

    def first_sends(step, _):
        begin(0, lax.rem(a + step, n_a), step)
        return 0

    def other_sends(step, _):
        for group in range(1, last + 1):
            begin(group, lax.rem(a + step, n_a), step)
        return 0

    def pack(i, _):
        z = 3 - i
        spread_plane(z)

        @pl.when(i == 0)
        def _():
            for code in range(1, 8):
                row_copy(code).wait_recv()
            own_row.wait()
            to_scalars = pltpu.make_async_copy(rows_ref, place, local.at[2])
            to_scalars.start()
            to_scalars.wait()

        emit_plane(z)

        @pl.when(i == 0)
        def _():
            lax.fori_loop(0, n_a, first_sends, 0)

        return 0

    lax.fori_loop(0, 4, pack, 0)
    own.start()
    lax.fori_loop(0, n_a, other_sends, 0)
    for code in range(1, 8):
        row_copy(code).wait_send()

    def arrived(source, mine_too):
        for group in range(last + 1):
            copy(group, 1, source, source).wait_recv()
            if groups[group][2]:
                copy(group, 0, source, source).wait_recv()
            elif mine_too:
                copy(group, 0, source, source).wait_recv()

    arrived(a, False)
    own.wait()

    def unpack(i, _):
        n = lax.rem(a + 2 * n_a - 1 - i, n_a)
        after = lax.rem(n + 1, n_a)

        @pl.when(i < n_a - 1)
        def _():
            arrived(n, True)

        def pair(step, _):
            g0 = jnp.minimum(2 * step, 7)
            arrays = []
            for z in range(4):
                for y in range(4):
                    here = r_ref[n, z, y, pl.ds(g0, 2)].reshape(8, 128)
                    there = r_ref[after, z, y, pl.ds(g0, 2)].reshape(8, 128)
                    arrays.append(jnp.where(mine, here, there))
            for bit in range(4):
                arrays = swap_bits(arrays, bit, 4 << bit)
            arrays = swap_bits(arrays, 2, 64)
            arrays = [jnp.take_along_axis(array, turn, axis=1, mode="promise_in_bounds") for array in arrays]
            for half in range(2):
                g = g0 + half
                vb = g // 3
                base = 4 * (g - 3 * vb) * 24 + 4 * vb
                for at in range(16):
                    thi, ri, m = at >> 3, (at >> 2) & 1, at & 3
                    sites[i, thi, pl.ds(base + ri * 12 + m, 4, stride=24)] = arrays[at][4 * half:4 * half + 4]
            return 0

        lax.fori_loop(0, 5, pair, 0)
        return 0

    def shipped(slot):
        n = lax.rem(a + 2 * n_a - 1 - slot, n_a)
        return pltpu.make_async_copy(sites.at[slot], out_ref.at[n], local.at[3 + slot])

    def four(quarter, _):
        lax.fori_loop(4 * quarter, 4 * quarter + 4, unpack, 0)

        def gram(h, _):
            def add(k, total):
                block = operand(sites, 4 * quarter, h * 6 + k)
                return total + lax.dot_general(block, block, (((1,), (1,)), ((), ())), precision=HIGH, preferred_element_type=jnp.float32)

            total = lax.fori_loop(0, 6, add, jnp.zeros((96, 96), jnp.float32)) / 1536.0
            total = jnp.concatenate([total, jnp.zeros((96, 32), jnp.float32)], axis=1)
            for i in range(4):
                n = lax.rem(a + 2 * n_a - 1 - (4 * quarter + i), n_a)
                piece = total[24 * i:24 * i + 24]
                if i:
                    piece = pltpu.roll(piece, 128 - 24 * i, 1)
                gram_ref[pl.ds(pl.multiple_of((h * 16 + n) * 24, 8), 24)] = piece
            return 0

        lax.fori_loop(0, 2, gram, 0)
        for i in range(4):
            shipped(4 * quarter + i).start()
        return 0

    lax.fori_loop(0, 4, four, 0)

    def sent(step, _):
        q = lax.rem(a + step, n_a)
        for group in range(last + 1):
            copy(group, 1, q, q).wait_send()
            if groups[group][2]:
                copy(group, 0, q, q).wait_send()
            else:
                pl.when(step > 0)(copy(group, 0, q, q).wait_send)
        shipped(step).wait()
        return 0

    lax.fori_loop(0, n_a, sent, 0)


def exchange(offsets, row, x, oz, oy):
    return pl.pallas_call(
        functools.partial(exchange_kernel, oz, oy),
        out_shape=[
            jax.ShapeDtypeStruct((16, 2, 288, 128), jnp.float32),
            jax.ShapeDtypeStruct((768, 128), jnp.float32),
        ],
        in_specs=[
            pl.BlockSpec(memory_space=pltpu.SMEM),
            pl.BlockSpec(memory_space=pltpu.VMEM),
            pl.BlockSpec(memory_space=pltpu.VMEM),
        ],
        out_specs=[pl.BlockSpec(memory_space=pl.ANY), pl.BlockSpec(memory_space=pltpu.VMEM)],
        scratch_shapes=[
            pltpu.SMEM((8, 1, 128), jnp.int32),
            pltpu.VMEM((8, 1, 128), jnp.int32),
            pltpu.VMEM((16 * 144, 128), jnp.float32),
            pltpu.VMEM((16, 4, 4, 9, 4, 128), jnp.float32),
            pltpu.VMEM((16, 4, 4, 9, 4, 128), jnp.float32),
            pltpu.VMEM((16, 2, 288, 128), jnp.float32),
            pltpu.SemaphoreType.DMA((3, 2, 16)),
            pltpu.SemaphoreType.DMA((3, 2, 16)),
            pltpu.SemaphoreType.DMA((8,)),
            pltpu.SemaphoreType.DMA((8,)),
            pltpu.SemaphoreType.DMA((19,)),
        ],
        compiler_params=pltpu.CompilerParams(has_side_effects=True, collective_id=3 * (oz - 1) + oy - 1),
        name=f"exchange_{oz}{oy}",
    )(offsets, row, x)


def per_device(near_null, offsets, owner_slot):
    spots = jnp.arange(128, dtype=jnp.int32)
    hits = owner_slot.reshape(16, 1) == spots[None, :]
    row = jnp.sum(jnp.where(hits, spots[:16, None], 0), axis=0, keepdims=True)
    x = near_null.transpose(0, 1, 3, 4, 2, 5).reshape(4, 4, 12, 48, 128)
    branches = [functools.partial(exchange, oz=oz, oy=oy) for oz in (1, 2, 3) for oy in (1, 2, 3)]
    sites, grams = lax.switch(3 * (offsets[1] - 1) + offsets[2] - 1, branches, offsets, row, x)
    return finish(grams, sites)


def solution(mesh):
    return jax.shard_map(
        per_device,
        mesh=mesh,
        in_specs=(P("ta", "gz", "gy", None, None, None), P(), P("ta", "gz", "gy", None)),
        out_specs=P(("ta", "gz", "gy"), None, None, None, None, None),
        check_vma=False,
    )
```

```python
import functools

import jax
import jax.numpy as jnp
from jax import lax
from jax.experimental import pallas as pl
from jax.experimental.pallas import tpu as pltpu
from jax.sharding import PartitionSpec as P

MESH = pl.DeviceIdType.MESH

HIGH = lax.Precision.HIGHEST
RIDGE = 0.05


def swap_bits(arrays, bit, distance):
    lanes = lax.broadcasted_iota(jnp.int32, arrays[0].shape, 1)
    low = (lanes & distance) == 0
    out = list(arrays)
    for first in range(len(arrays)):
        if first & (1 << bit):
            continue
        second = first | (1 << bit)
        a, b = arrays[first], arrays[second]
        out[first] = jnp.where(low, a, pltpu.roll(b, distance, 1))
        out[second] = jnp.where(low, pltpu.roll(a, 128 - distance, 1), b)
    return out


def cmul_sub(ar, ai, br, bi, cr, ci):
    return ar - (br * cr - bi * ci), ai - (br * ci + bi * cr)


def factor(gr, gi, rows):
    gr, gi = list(gr), list(gi)
    diag = gr[0][0:1]
    for v in range(1, 12):
        diag = diag + gr[v][v:v + 1]
    ridge = RIDGE * (diag / 12.0 + 1e-06)
    low_r, low_i, inv = [None] * 12, [None] * 12, [None] * 12
    for j in range(12):
        d = jnp.sqrt(gr[j][j:j + 1] + ridge)
        inv[j] = 1.0 / d
        below = rows > j
        low_r[j] = jnp.where(below, gr[j] * inv[j], 0.0)
        low_i[j] = jnp.where(below, gi[j] * inv[j], 0.0)
        for w in range(j + 1, 12):
            wr, wi = low_r[j][w:w + 1], low_i[j][w:w + 1]
            gr[w] = gr[w] - (low_r[j] * wr + low_i[j] * wi)
            gi[w] = gi[w] - (low_i[j] * wr - low_r[j] * wi)
    xr, xi = [], []
    for c in range(12):
        ar = jnp.where(rows == c, inv[c], 0.0)
        ai = jnp.zeros_like(ar)
        for m in range(c, 12):
            if m > c:
                here = rows == m
                ar = jnp.where(here, ar * inv[m], ar)
                ai = jnp.where(here, ai * inv[m], ai)
            if m < 11:
                ar, ai = cmul_sub(ar, ai, low_r[m], low_i[m], ar[m:m + 1], ai[m:m + 1])
        xr.append(ar)
        xi.append(ai)
    return xr, xi


def small_product(ar, ai, entry, span):
    out_r, out_i = [], []
    for c in range(12):
        sr = si = None
        for l in span(c):
            er, ei = entry(l, c)
            tr = ar[l] * er - ai[l] * ei
            ti = ar[l] * ei + ai[l] * er
            sr, si = (tr, ti) if sr is None else (sr + tr, si + ti)
        out_r.append(sr)
        out_i.append(si)
    return out_r, out_i


def split(x):
    first = x.astype(jnp.bfloat16)
    rest = x - first.astype(jnp.float32)
    second = rest.astype(jnp.bfloat16)
    return first, second, (rest - second.astype(jnp.float32)).astype(jnp.bfloat16)


def product(left, right, at):
    return lax.dot_general(left, right, (((1,), (at,)), ((), ())), preferred_element_type=jnp.float32)


def operand(ref, first, c):
    rows = pl.ds(pl.multiple_of(c * 24, 8), 24)
    parts = [ref[pl.ds(first, 4), thi, rows].reshape(96, 128) for thi in range(2)]
    return jnp.concatenate(parts, axis=1)


def finish_kernel(gram_ref, sites_ref, o_ref, maps):
    step = pl.program_id(0)
    lane128 = lax.broadcasted_iota(jnp.int32, (24, 128), 1)

    @pl.when(step == 0)
    def _():
        columns = []
        for four in range(6):
            stack = jnp.concatenate([gram_ref[pl.ds(4 * four + i, 32, stride=24)] for i in range(4)], axis=0)
            turned = jnp.transpose(stack)[0:24]
            for i in range(4):
                columns.append(pltpu.roll(turned, 128 - 32 * i, 1) if i else turned)
        columns = [jnp.where(lane128 < 32, column, 0.0) for column in columns]
        rows = lax.broadcasted_iota(jnp.int32, (12, 128), 0)
        gr = [columns[w][0:12] + columns[12 + w][12:24] for w in range(12)]
        gi = [columns[12 + w][0:12] - columns[w][12:24] for w in range(12)]
        xr, xi = factor(gr, gi, rows)
        tr, ti = small_product(xr, xi, lambda l, c: (gr[c][l:l + 1], gi[c][l:l + 1]), lambda c: range(12))
        sr, si = small_product(tr, ti, lambda l, c: (xr[l][c:c + 1], -xi[l][c:c + 1]), lambda c: range(c + 1))
        yr, yi = factor(sr, si, rows)
        mr, mi = small_product(yr, yi, lambda l, c: (xr[c][l:l + 1], xi[c][l:l + 1]), lambda c: range(c, 12))
        for four in range(6):
            stack = None
            for i in range(4):
                r = 4 * four + i
                v = r % 12
                column = jnp.concatenate([mr[v], -mi[v]] if r < 12 else [mi[v], mr[v]], axis=0)
                column = jnp.where(lane128 < 32, column, 0.0)
                if i:
                    column = pltpu.roll(column, 32 * i, 1)
                stack = column if stack is None else stack + column
            stack = jnp.concatenate([stack, jnp.zeros((104, 128), jnp.float32)], axis=0)
            turned = jnp.transpose(stack)
            for i in range(4):
                maps[pl.ds(4 * four + i, 32, stride=24)] = turned[32 * i:32 * i + 32]

    for h in range(2):
        parts = []
        for i in range(4):
            piece = maps[pl.ds(pl.multiple_of((h * 16 + 4 * step + i) * 24, 8), 24)]
            parts.append(pltpu.roll(piece, 24 * i, 1) if i else piece)
        parts.append(jnp.zeros((32, 128), jnp.float32))
        mixing = jnp.transpose(jnp.concatenate(parts, axis=0))[0:96]
        a1, a2, a3 = split(mixing)
        left = jnp.concatenate([a1, a2], axis=1)
        right = jnp.concatenate([a1, a3], axis=1)
        still = jnp.zeros((32, 256), jnp.bfloat16)

        def one(k, _):
            b1, b2, b3 = split(operand(sites_ref, 0, h * 6 + k))
            b1, b2, b3 = [jnp.concatenate([b, still], axis=0) for b in (b1, b2, b3)]
            out = product(right, jnp.concatenate([b3, b1], axis=0), 0)
            out = out + product(left, jnp.concatenate([b2, b2], axis=0), 0)
            out = out + product(left, jnp.concatenate([b1, b1], axis=0), 0)
            for i in range(4):
                for ri in range(2):
                    for col in range(2):
                        start = ((i * 2 + h) * 12) * 24 + k * 4 + col * 2 + ri
                        o_ref[pl.ds(start, 12, stride=24)] = out[24 * i + 12 * ri:24 * i + 12 * ri + 12, 128 * col:128 * col + 128]
            return 0

        lax.fori_loop(0, 6, one, 0, unroll=6)


def finish(grams, sites):
    out = pl.pallas_call(
        finish_kernel,
        out_shape=jax.ShapeDtypeStruct((9216, 128), jnp.float32),
        grid=(4,),
        in_specs=[
            pl.BlockSpec((768, 128), lambda i: (0, 0)),
            pl.BlockSpec((4, 2, 288, 128), lambda i: (i, 0, 0, 0)),
        ],
        out_specs=pl.BlockSpec((2304, 128), lambda i: (i, 0)),
        scratch_shapes=[pltpu.VMEM((768, 128), jnp.float32)],
        compiler_params=pltpu.CompilerParams(dimension_semantics=("arbitrary",)),
        name="finish",
    )(grams, sites)
    out = out.reshape(16, 2, 12, 6, 2, 2, 128)
    return out.transpose(0, 1, 2, 3, 5, 4, 6).reshape(16, 2, 12, 6, 2, 256)


def exchange_kernel(oz, oy, off_ref, row_ref, x_hbm, out_ref, gram_ref, x_ref, place, rows_ref, tiles, s_ref, r_ref, sites, send, recv, row_send, row_recv, local, loads):
    a, b, c = lax.axis_index("ta"), lax.axis_index("gz"), lax.axis_index("gy")
    n_a, n_b, n_c = lax.axis_size("ta"), lax.axis_size("gz"), lax.axis_size("gy")
    ot, ox = off_ref[0], off_ref[3]
    spans = ((0, 4 - oy), (4 - oy, oy))
    groups = ((3, 1, 1),) + {1: ((0, 3, 0),), 2: ((2, 1, 1), (0, 2, 0)), 3: ((1, 2, 1), (0, 1, 0))}[oz]

    def peer(code, sign):
        da, db, dc = (code >> 2) & 1, (code >> 1) & 1, code & 1
        return (lax.rem(a + n_a + sign * da, n_a), lax.rem(b + n_b + sign * db, n_b), lax.rem(c + n_c + sign * dc, n_c))

    def load(z):
        from_z = lax.rem(z + oz, 4)
        return pltpu.make_async_copy(x_hbm.at[:, from_z], x_ref.at[:, from_z], loads.at[z])

    for i in range(4):
        load(3 - i).start()

    barrier = pltpu.get_barrier_semaphore()

    def greet(step, _):
        q = lax.rem(a + step, n_a)
        for code in (3, 2, 1):
            device = (q,) + peer(code, 1)[1:]
            pl.semaphore_signal(barrier, inc=1, device_id=device, device_id_type=MESH)

        @pl.when(step > 0)
        def _():
            pl.semaphore_signal(barrier, inc=1, device_id=(q, b, c), device_id_type=MESH)

        return 0

    for code in (1, 2, 3, 5, 6, 7):
        pl.semaphore_signal(barrier, inc=1, device_id=peer(code, -1), device_id_type=MESH)
    lax.fori_loop(0, n_a, greet, 0)
    pl.semaphore_wait(barrier, 4 * n_a + 5)

    def row_copy(code):
        return pltpu.make_async_remote_copy(
            row_ref,
            rows_ref.at[code],
            row_send.at[code],
            row_recv.at[code],
            device_id=peer(code, 1),
            device_id_type=MESH,
        )

    own_row = pltpu.make_async_copy(row_ref, rows_ref.at[0], local.at[0])
    own_row.start()
    for code in range(1, 8):
        row_copy(code).start()

    lanes = lax.broadcasted_iota(jnp.int32, (8, 128), 1)
    stays = (lanes & 3) >= ox
    turn = (lanes & 124) | ((lanes + ox) & 3)
    mine = ((lanes >> 4) & 3) < 4 - ot
    mine4 = ((lax.broadcasted_iota(jnp.int32, (4, 128), 1) >> 4) & 3) < 4 - ot

    def copy(group, dy, q, lands):
        z0, nz, dz = groups[group]
        y0, ny = spans[dy]
        return pltpu.make_async_remote_copy(
            s_ref.at[q, pl.ds(z0, nz), pl.ds(y0, ny)],
            r_ref.at[lands, pl.ds(z0, nz), pl.ds(y0, ny)],
            send.at[group, dy, q],
            recv.at[group, dy, lands],
            device_id=(q, lax.rem(b + n_b - dz, n_b), lax.rem(c + n_c - dy, n_c)),
            device_id_type=MESH,
        )

    last = len(groups) - 1
    z_own, nz_own, _ = groups[last]
    own = pltpu.make_async_copy(
        s_ref.at[a, pl.ds(z_own, nz_own), pl.ds(0, 4 - oy)],
        r_ref.at[a, pl.ds(z_own, nz_own), pl.ds(0, 4 - oy)],
        local.at[1],
    )

    def spread_plane(z):
        from_z = lax.rem(z + oz, 4)
        def spread(step, _):
            vb, part = step // 6, lax.rem(step, 6)
            rows = pl.ds(pl.multiple_of(8 * part, 8), 8)
            arrays = [x_ref[(t + ot) & 3, from_z, 4 * vb + m, rows] for t in range(4) for m in range(4)]
            for bit in range(4):
                arrays = swap_bits(arrays, bit, 4 << bit)
            for j in range(16):
                row = pl.multiple_of(j * 144 + vb * 48 + 8 * part, 8)
                tiles[pl.ds(row, 8)] = jnp.where(stays, arrays[j], arrays[(j + 1) % 16])
            return 0

        lax.fori_loop(0, 18, spread, 0, unroll=3)

    def emit_plane(z, after_one=None):
        dz = (z + oz) // 4

        def emit(step, _):
            q = lax.rem(a + step, n_a)
            for y in range(4):
                home = 2 * dz + (y + oy) // 4
                first = place[home, 0, q] * 144 + (y + oy) % 4
                second = place[4 + home, 0, q] * 144 + (y + oy) % 4
                for g in range(9):
                    s_ref[q, z, y, g] = jnp.where(
                        mine4,
                        tiles[pl.ds(first + 16 * g, 4, stride=4)],
                        tiles[pl.ds(second + 16 * g, 4, stride=4)],
                    )
            if after_one is not None:
                pl.when(step > 0)(functools.partial(after_one, step - 1))
            return 0

        lax.fori_loop(0, n_a, emit, 0, unroll=1)
        if after_one is not None:
            after_one(n_a - 1)

    def begin(group, q, step):
        copy(group, 1, q, a).start()
        if groups[group][2]:
            copy(group, 0, q, a).start()
        else:
            pl.when(step > 0)(copy(group, 0, q, a).start)

    def first_send(step):
        begin(0, lax.rem(a + step, n_a), step)

    def other_sends(step, _):
        for group in range(1, last + 1):
            begin(group, lax.rem(a + step, n_a), step)
        return 0

    for i in range(4):
        load(i).wait()
    spread_plane(3)
    for code in range(1, 8):
        row_copy(code).wait_recv()
    own_row.wait()
    to_scalars = pltpu.make_async_copy(rows_ref, place, local.at[2])
    to_scalars.start()
    to_scalars.wait()
    emit_plane(3, first_send)

    def pack(i, _):
        spread_plane(2 - i)
        emit_plane(2 - i)
        return 0

    lax.fori_loop(0, 3, pack, 0)
    own.start()
    lax.fori_loop(0, n_a, other_sends, 0)
    for code in range(1, 8):
        row_copy(code).wait_send()

    def arrived(source, mine_too):
        for group in range(last + 1):
            copy(group, 1, source, source).wait_recv()
            if groups[group][2]:
                copy(group, 0, source, source).wait_recv()
            elif mine_too:
                copy(group, 0, source, source).wait_recv()

    arrived(a, False)
    own.wait()

    def shipped(slot):
        n = lax.rem(a + 2 * n_a - 1 - slot, n_a)
        return pltpu.make_async_copy(sites.at[slot], out_ref.at[n], local.at[3 + slot])

    def unpack(i, _):
        n = lax.rem(a + 2 * n_a - 1 - i, n_a)
        after = lax.rem(n + 1, n_a)

        @pl.when(i < n_a - 1)
        def _():
            arrived(n, True)

        def pair(step, _):
            g0 = jnp.minimum(2 * step, 7)
            arrays = []
            for z in range(4):
                for y in range(4):
                    here = r_ref[n, z, y, pl.ds(g0, 2)].reshape(8, 128)
                    there = r_ref[after, z, y, pl.ds(g0, 2)].reshape(8, 128)
                    arrays.append(jnp.where(mine, here, there))
            for bit in range(4):
                arrays = swap_bits(arrays, bit, 4 << bit)
            arrays = swap_bits(arrays, 2, 64)
            arrays = [jnp.take_along_axis(array, turn, axis=1, mode="promise_in_bounds") for array in arrays]
            for half in range(2):
                g = g0 + half
                vb = g // 3
                base = 4 * (g - 3 * vb) * 24 + 4 * vb
                for at in range(16):
                    thi, ri, m = at >> 3, (at >> 2) & 1, at & 3
                    sites[i, thi, pl.ds(base + ri * 12 + m, 4, stride=24)] = arrays[at][4 * half:4 * half + 4]
            return 0

        lax.fori_loop(0, 5, pair, 0, unroll=5)
        pl.when(i > 0)(lambda: shipped(i - 1).start())
        return 0

    def four(quarter, _):
        lax.fori_loop(4 * quarter, 4 * quarter + 4, unpack, 0)

        def gram(h, _):
            def add(k, total):
                block = operand(sites, 4 * quarter, h * 6 + k)
                return total + lax.dot_general(block, block, (((1,), (1,)), ((), ())), precision=HIGH, preferred_element_type=jnp.float32)

            total = lax.fori_loop(0, 6, add, jnp.zeros((96, 96), jnp.float32), unroll=6) / 1536.0
            total = jnp.concatenate([total, jnp.zeros((96, 32), jnp.float32)], axis=1)
            for i in range(4):
                n = lax.rem(a + 2 * n_a - 1 - (4 * quarter + i), n_a)
                piece = total[24 * i:24 * i + 24]
                if i:
                    piece = pltpu.roll(piece, 128 - 24 * i, 1)
                gram_ref[pl.ds(pl.multiple_of((h * 16 + n) * 24, 8), 24)] = piece
            return 0

        lax.fori_loop(0, 2, gram, 0)
        return 0

    lax.fori_loop(0, 4, four, 0)
    shipped(n_a - 1).start()

    def sent(step, _):
        q = lax.rem(a + step, n_a)
        for group in range(last + 1):
            copy(group, 1, q, q).wait_send()
            if groups[group][2]:
                copy(group, 0, q, q).wait_send()
            else:
                pl.when(step > 0)(copy(group, 0, q, q).wait_send)
        shipped(step).wait()
        return 0

    lax.fori_loop(0, n_a, sent, 0)


def exchange(offsets, row, x, oz, oy):
    return pl.pallas_call(
        functools.partial(exchange_kernel, oz, oy),
        out_shape=[
            jax.ShapeDtypeStruct((16, 2, 288, 128), jnp.float32),
            jax.ShapeDtypeStruct((768, 128), jnp.float32),
        ],
        in_specs=[
            pl.BlockSpec(memory_space=pltpu.SMEM),
            pl.BlockSpec(memory_space=pltpu.VMEM),
            pl.BlockSpec(memory_space=pl.ANY),
        ],
        out_specs=[pl.BlockSpec(memory_space=pl.ANY), pl.BlockSpec(memory_space=pltpu.VMEM)],
        scratch_shapes=[
            pltpu.VMEM((4, 4, 12, 48, 128), jnp.float32),
            pltpu.SMEM((8, 1, 128), jnp.int32),
            pltpu.VMEM((8, 1, 128), jnp.int32),
            pltpu.VMEM((16 * 144, 128), jnp.float32),
            pltpu.VMEM((16, 4, 4, 9, 4, 128), jnp.float32),
            pltpu.VMEM((16, 4, 4, 9, 4, 128), jnp.float32),
            pltpu.VMEM((16, 2, 288, 128), jnp.float32),
            pltpu.SemaphoreType.DMA((3, 2, 16)),
            pltpu.SemaphoreType.DMA((3, 2, 16)),
            pltpu.SemaphoreType.DMA((8,)),
            pltpu.SemaphoreType.DMA((8,)),
            pltpu.SemaphoreType.DMA((19,)),
            pltpu.SemaphoreType.DMA((4,)),
        ],
        compiler_params=pltpu.CompilerParams(has_side_effects=True, collective_id=3 * (oz - 1) + oy - 1),
        name=f"exchange_{oz}{oy}",
    )(offsets, row, x)


def per_device(near_null, offsets, owner_slot):
    spots = jnp.arange(128, dtype=jnp.int32)
    hits = owner_slot.reshape(16, 1) == spots[None, :]
    row = jnp.sum(jnp.where(hits, spots[:16, None], 0), axis=0, keepdims=True)
    x = near_null.transpose(0, 1, 3, 4, 2, 5).reshape(4, 4, 12, 48, 128)
    branches = [functools.partial(exchange, oz=oz, oy=oy) for oz in (1, 2, 3) for oy in (1, 2, 3)]
    sites, grams = lax.switch(3 * (offsets[1] - 1) + offsets[2] - 1, branches, offsets, row, x)
    return finish(grams, sites)


def solution(mesh):
    return jax.shard_map(
        per_device,
        mesh=mesh,
        in_specs=(P("ta", "gz", "gy", None, None, None), P(), P("ta", "gz", "gy", None)),
        out_specs=P(("ta", "gz", "gy"), None, None, None, None, None),
        check_vma=False,
    )
```

```python
import functools

import jax
import jax.numpy as jnp
from jax import lax
from jax.experimental import pallas as pl
from jax.experimental.pallas import tpu as pltpu
from jax.sharding import PartitionSpec as P

MESH = pl.DeviceIdType.MESH

HIGH = lax.Precision.HIGHEST
RIDGE = 0.05


def swap_bits(arrays, bit, distance):
    lanes = lax.broadcasted_iota(jnp.int32, arrays[0].shape, 1)
    low = (lanes & distance) == 0
    out = list(arrays)
    for first in range(len(arrays)):
        if first & (1 << bit):
            continue
        second = first | (1 << bit)
        a, b = arrays[first], arrays[second]
        out[first] = jnp.where(low, a, pltpu.roll(b, distance, 1))
        out[second] = jnp.where(low, pltpu.roll(a, 128 - distance, 1), b)
    return out


def cmul_sub(ar, ai, br, bi, cr, ci):
    return ar - (br * cr - bi * ci), ai - (br * ci + bi * cr)


def factor(gr, gi, rows):
    gr, gi = list(gr), list(gi)
    diag = gr[0][0:1]
    for v in range(1, 12):
        diag = diag + gr[v][v:v + 1]
    ridge = RIDGE * (diag / 12.0 + 1e-06)
    low_r, low_i, inv = [None] * 12, [None] * 12, [None] * 12
    for j in range(12):
        d = jnp.sqrt(gr[j][j:j + 1] + ridge)
        inv[j] = 1.0 / d
        below = rows > j
        low_r[j] = jnp.where(below, gr[j] * inv[j], 0.0)
        low_i[j] = jnp.where(below, gi[j] * inv[j], 0.0)
        for w in range(j + 1, 12):
            wr, wi = low_r[j][w:w + 1], low_i[j][w:w + 1]
            gr[w] = gr[w] - (low_r[j] * wr + low_i[j] * wi)
            gi[w] = gi[w] - (low_i[j] * wr - low_r[j] * wi)
    xr, xi = [], []
    for c in range(12):
        ar = jnp.where(rows == c, inv[c], 0.0)
        ai = jnp.zeros_like(ar)
        for m in range(c, 12):
            if m > c:
                here = rows == m
                ar = jnp.where(here, ar * inv[m], ar)
                ai = jnp.where(here, ai * inv[m], ai)
            if m < 11:
                ar, ai = cmul_sub(ar, ai, low_r[m], low_i[m], ar[m:m + 1], ai[m:m + 1])
        xr.append(ar)
        xi.append(ai)
    return xr, xi


def small_product(ar, ai, entry, span):
    out_r, out_i = [], []
    for c in range(12):
        sr = si = None
        for l in span(c):
            er, ei = entry(l, c)
            tr = ar[l] * er - ai[l] * ei
            ti = ar[l] * ei + ai[l] * er
            sr, si = (tr, ti) if sr is None else (sr + tr, si + ti)
        out_r.append(sr)
        out_i.append(si)
    return out_r, out_i


def split(x):
    first = x.astype(jnp.bfloat16)
    rest = x - first.astype(jnp.float32)
    second = rest.astype(jnp.bfloat16)
    return first, second, (rest - second.astype(jnp.float32)).astype(jnp.bfloat16)


def product(left, right, at):
    return lax.dot_general(left, right, (((1,), (at,)), ((), ())), preferred_element_type=jnp.float32)


def operand(ref, first, c):
    rows = pl.ds(pl.multiple_of(c * 24, 8), 24)
    parts = [ref[pl.ds(first, 4), thi, rows].reshape(96, 128) for thi in range(2)]
    return jnp.concatenate(parts, axis=1)


def finish_kernel(gram_ref, sites_ref, o_ref, maps):
    step = pl.program_id(0)
    lane128 = lax.broadcasted_iota(jnp.int32, (24, 128), 1)

    @pl.when(step == 0)
    def _():
        columns = []
        for four in range(6):
            stack = jnp.concatenate([gram_ref[pl.ds(4 * four + i, 32, stride=24)] for i in range(4)], axis=0)
            turned = jnp.transpose(stack)[0:24]
            for i in range(4):
                columns.append(pltpu.roll(turned, 128 - 32 * i, 1) if i else turned)
        columns = [jnp.where(lane128 < 32, column, 0.0) for column in columns]
        rows = lax.broadcasted_iota(jnp.int32, (12, 128), 0)
        gr = [columns[w][0:12] + columns[12 + w][12:24] for w in range(12)]
        gi = [columns[12 + w][0:12] - columns[w][12:24] for w in range(12)]
        xr, xi = factor(gr, gi, rows)
        tr, ti = small_product(xr, xi, lambda l, c: (gr[c][l:l + 1], gi[c][l:l + 1]), lambda c: range(12))
        sr, si = small_product(tr, ti, lambda l, c: (xr[l][c:c + 1], -xi[l][c:c + 1]), lambda c: range(c + 1))
        yr, yi = factor(sr, si, rows)
        mr, mi = small_product(yr, yi, lambda l, c: (xr[c][l:l + 1], xi[c][l:l + 1]), lambda c: range(c, 12))
        for four in range(6):
            stack = None
            for i in range(4):
                r = 4 * four + i
                v = r % 12
                column = jnp.concatenate([mr[v], -mi[v]] if r < 12 else [mi[v], mr[v]], axis=0)
                column = jnp.where(lane128 < 32, column, 0.0)
                if i:
                    column = pltpu.roll(column, 32 * i, 1)
                stack = column if stack is None else stack + column
            stack = jnp.concatenate([stack, jnp.zeros((104, 128), jnp.float32)], axis=0)
            turned = jnp.transpose(stack)
            for i in range(4):
                maps[pl.ds(4 * four + i, 32, stride=24)] = turned[32 * i:32 * i + 32]

    for h in range(2):
        parts = []
        for i in range(4):
            piece = maps[pl.ds(pl.multiple_of((h * 16 + 4 * step + i) * 24, 8), 24)]
            parts.append(pltpu.roll(piece, 24 * i, 1) if i else piece)
        parts.append(jnp.zeros((32, 128), jnp.float32))
        mixing = jnp.transpose(jnp.concatenate(parts, axis=0))[0:96]
        a1, a2, a3 = split(mixing)
        left = jnp.concatenate([a1, a2], axis=1)
        right = jnp.concatenate([a1, a3], axis=1)
        still = jnp.zeros((32, 256), jnp.bfloat16)

        def one(k, _):
            b1, b2, b3 = split(operand(sites_ref, 0, h * 6 + k))
            b1, b2, b3 = [jnp.concatenate([b, still], axis=0) for b in (b1, b2, b3)]
            out = product(right, jnp.concatenate([b3, b1], axis=0), 0)
            out = out + product(left, jnp.concatenate([b2, b2], axis=0), 0)
            out = out + product(left, jnp.concatenate([b1, b1], axis=0), 0)
            for i in range(4):
                for ri in range(2):
                    for col in range(2):
                        start = ((i * 2 + h) * 12) * 24 + k * 4 + col * 2 + ri
                        o_ref[pl.ds(start, 12, stride=24)] = out[24 * i + 12 * ri:24 * i + 12 * ri + 12, 128 * col:128 * col + 128]
            return 0

        lax.fori_loop(0, 6, one, 0, unroll=6)


def finish(grams, sites):
    out = pl.pallas_call(
        finish_kernel,
        out_shape=jax.ShapeDtypeStruct((9216, 128), jnp.float32),
        grid=(4,),
        in_specs=[
            pl.BlockSpec((768, 128), lambda i: (0, 0)),
            pl.BlockSpec((4, 2, 288, 128), lambda i: (i, 0, 0, 0)),
        ],
        out_specs=pl.BlockSpec((2304, 128), lambda i: (i, 0)),
        scratch_shapes=[pltpu.VMEM((768, 128), jnp.float32)],
        compiler_params=pltpu.CompilerParams(dimension_semantics=("arbitrary",)),
        name="finish",
    )(grams, sites)
    out = out.reshape(16, 2, 12, 6, 2, 2, 128)
    return out.transpose(0, 1, 2, 3, 5, 4, 6).reshape(16, 2, 12, 6, 2, 256)


def exchange_kernel(oz, oy, off_ref, slot_ref, x_hbm, out_ref, gram_ref, x_ref, row_ref, place, rows_ref, tiles, s_ref, r_ref, sites, send, recv, row_send, row_recv, local, loads):
    a, b, c = lax.axis_index("ta"), lax.axis_index("gz"), lax.axis_index("gy")
    n_a, n_b, n_c = lax.axis_size("ta"), lax.axis_size("gz"), lax.axis_size("gy")
    ot, ox = off_ref[0], off_ref[3]
    spans = ((0, 4 - oy), (4 - oy, oy))
    groups = ((3, 1, 1),) + {1: ((0, 3, 0),), 2: ((2, 1, 1), (0, 2, 0)), 3: ((1, 2, 1), (0, 1, 0))}[oz]

    def peer(code, sign):
        da, db, dc = (code >> 2) & 1, (code >> 1) & 1, code & 1
        return (lax.rem(a + n_a + sign * da, n_a), lax.rem(b + n_b + sign * db, n_b), lax.rem(c + n_c + sign * dc, n_c))

    def load(z):
        from_z = lax.rem(z + oz, 4)
        return pltpu.make_async_copy(x_hbm.at[:, from_z], x_ref.at[:, from_z], loads.at[z])

    barrier = pltpu.get_barrier_semaphore()

    def greet(step, _):
        q = lax.rem(a + step, n_a)
        for code in (3, 2, 1):
            device = (q,) + peer(code, 1)[1:]
            pl.semaphore_signal(barrier, inc=1, device_id=device, device_id_type=MESH)

        @pl.when(step > 0)
        def _():
            pl.semaphore_signal(barrier, inc=1, device_id=(q, b, c), device_id_type=MESH)

        return 0

    for code in (1, 2, 3, 5, 6, 7):
        pl.semaphore_signal(barrier, inc=1, device_id=peer(code, -1), device_id_type=MESH)
    lax.fori_loop(0, n_a, greet, 0)
    for i in range(4):
        load(3 - i).start()
    spots = lax.broadcasted_iota(jnp.int32, (1, 128), 1)
    row = jnp.zeros((1, 128), jnp.int32)
    for j in range(16):
        row = jnp.where(spots == slot_ref[j], j, row)
    row_ref[...] = row
    pl.semaphore_wait(barrier, 4 * n_a + 5)

    def row_copy(code):
        return pltpu.make_async_remote_copy(
            row_ref,
            rows_ref.at[code],
            row_send.at[code],
            row_recv.at[code],
            device_id=peer(code, 1),
            device_id_type=MESH,
        )

    own_row = pltpu.make_async_copy(row_ref, rows_ref.at[0], local.at[0])
    own_row.start()
    for code in range(1, 8):
        row_copy(code).start()

    lanes = lax.broadcasted_iota(jnp.int32, (8, 128), 1)
    stays = (lanes & 3) >= ox
    turn = (lanes & 124) | ((lanes + ox) & 3)
    mine = ((lanes >> 4) & 3) < 4 - ot
    mine4 = ((lax.broadcasted_iota(jnp.int32, (4, 128), 1) >> 4) & 3) < 4 - ot

    def copy(group, dy, q, lands):
        z0, nz, dz = groups[group]
        y0, ny = spans[dy]
        return pltpu.make_async_remote_copy(
            s_ref.at[q, pl.ds(z0, nz), pl.ds(y0, ny)],
            r_ref.at[lands, pl.ds(z0, nz), pl.ds(y0, ny)],
            send.at[group, dy, q],
            recv.at[group, dy, lands],
            device_id=(q, lax.rem(b + n_b - dz, n_b), lax.rem(c + n_c - dy, n_c)),
            device_id_type=MESH,
        )

    last = len(groups) - 1
    z_own, nz_own, _ = groups[last]
    own = pltpu.make_async_copy(
        s_ref.at[a, pl.ds(z_own, nz_own), pl.ds(0, 4 - oy)],
        r_ref.at[a, pl.ds(z_own, nz_own), pl.ds(0, 4 - oy)],
        local.at[1],
    )

    def spread_plane(z):
        from_z = lax.rem(z + oz, 4)
        def spread(step, _):
            vb, part = step // 6, lax.rem(step, 6)
            rows = pl.ds(pl.multiple_of(8 * part, 8), 8)
            arrays = [x_ref[(t + ot) & 3, from_z, 4 * vb + m, rows] for t in range(4) for m in range(4)]
            for bit in range(4):
                arrays = swap_bits(arrays, bit, 4 << bit)
            for j in range(16):
                row = pl.multiple_of(j * 144 + vb * 48 + 8 * part, 8)
                tiles[pl.ds(row, 8)] = jnp.where(stays, arrays[j], arrays[(j + 1) % 16])
            return 0

        lax.fori_loop(0, 18, spread, 0, unroll=3)

    def emit_plane(z, after_one=None):
        dz = (z + oz) // 4

        def emit(step, _):
            q = lax.rem(a + step, n_a)
            for y in range(4):
                home = 2 * dz + (y + oy) // 4
                first = place[home, 0, q] * 144 + (y + oy) % 4
                second = place[4 + home, 0, q] * 144 + (y + oy) % 4
                for g in range(9):
                    s_ref[q, z, y, g] = jnp.where(
                        mine4,
                        tiles[pl.ds(first + 16 * g, 4, stride=4)],
                        tiles[pl.ds(second + 16 * g, 4, stride=4)],
                    )
            if after_one is not None:
                pl.when(step > 0)(functools.partial(after_one, step - 1))
            return 0

        lax.fori_loop(0, n_a, emit, 0, unroll=1)
        if after_one is not None:
            after_one(n_a - 1)

    def begin(group, q, step):
        copy(group, 1, q, a).start()
        if groups[group][2]:
            copy(group, 0, q, a).start()
        else:
            pl.when(step > 0)(copy(group, 0, q, a).start)

    def first_send(step):
        begin(0, lax.rem(a + step, n_a), step)

    def other_sends(step, _):
        for group in range(1, last + 1):
            begin(group, lax.rem(a + step, n_a), step)
        return 0

    for i in range(4):
        load(i).wait()
    spread_plane(3)
    for code in range(1, 8):
        row_copy(code).wait_recv()
    own_row.wait()
    to_scalars = pltpu.make_async_copy(rows_ref, place, local.at[2])
    to_scalars.start()
    to_scalars.wait()
    emit_plane(3, first_send)

    def pack(i, _):
        spread_plane(2 - i)
        emit_plane(2 - i)
        return 0

    lax.fori_loop(0, 3, pack, 0)
    own.start()
    lax.fori_loop(0, n_a, other_sends, 0)
    for code in range(1, 8):
        row_copy(code).wait_send()

    def arrived(source, mine_too):
        for group in range(last + 1):
            copy(group, 1, source, source).wait_recv()
            if groups[group][2]:
                copy(group, 0, source, source).wait_recv()
            elif mine_too:
                copy(group, 0, source, source).wait_recv()

    arrived(a, False)
    own.wait()

    def shipped(slot):
        n = lax.rem(a + 2 * n_a - 1 - slot, n_a)
        return pltpu.make_async_copy(sites.at[slot], out_ref.at[n], local.at[3 + slot])

    def unpack(i, _):
        n = lax.rem(a + 2 * n_a - 1 - i, n_a)
        after = lax.rem(n + 1, n_a)

        @pl.when(i < n_a - 1)
        def _():
            arrived(n, True)

        def pair(step, _):
            g0 = jnp.minimum(2 * step, 7)
            arrays = []
            for z in range(4):
                for y in range(4):
                    here = r_ref[n, z, y, pl.ds(g0, 2)].reshape(8, 128)
                    there = r_ref[after, z, y, pl.ds(g0, 2)].reshape(8, 128)
                    arrays.append(jnp.where(mine, here, there))
            for bit in range(4):
                arrays = swap_bits(arrays, bit, 4 << bit)
            arrays = swap_bits(arrays, 2, 64)
            arrays = [jnp.take_along_axis(array, turn, axis=1, mode="promise_in_bounds") for array in arrays]
            for half in range(2):
                g = g0 + half
                vb = g // 3
                base = 4 * (g - 3 * vb) * 24 + 4 * vb
                for at in range(16):
                    thi, ri, m = at >> 3, (at >> 2) & 1, at & 3
                    sites[i, thi, pl.ds(base + ri * 12 + m, 4, stride=24)] = arrays[at][4 * half:4 * half + 4]
            return 0

        lax.fori_loop(0, 5, pair, 0, unroll=5)
        pl.when(i > 0)(lambda: shipped(i - 1).start())
        return 0

    def four(quarter, _):
        lax.fori_loop(4 * quarter, 4 * quarter + 4, unpack, 0)

        def gram(h, _):
            def add(k, total):
                block = operand(sites, 4 * quarter, h * 6 + k)
                return total + lax.dot_general(block, block, (((1,), (1,)), ((), ())), precision=HIGH, preferred_element_type=jnp.float32)

            total = lax.fori_loop(0, 6, add, jnp.zeros((96, 96), jnp.float32), unroll=6) / 1536.0
            total = jnp.concatenate([total, jnp.zeros((96, 32), jnp.float32)], axis=1)
            for i in range(4):
                n = lax.rem(a + 2 * n_a - 1 - (4 * quarter + i), n_a)
                piece = total[24 * i:24 * i + 24]
                if i:
                    piece = pltpu.roll(piece, 128 - 24 * i, 1)
                gram_ref[pl.ds(pl.multiple_of((h * 16 + n) * 24, 8), 24)] = piece
            return 0

        lax.fori_loop(0, 2, gram, 0)
        return 0

    lax.fori_loop(0, 4, four, 0)
    shipped(n_a - 1).start()

    def sent(step, _):
        q = lax.rem(a + step, n_a)
        for group in range(last + 1):
            copy(group, 1, q, q).wait_send()
            if groups[group][2]:
                copy(group, 0, q, q).wait_send()
            else:
                pl.when(step > 0)(copy(group, 0, q, q).wait_send)
        shipped(step).wait()
        return 0

    lax.fori_loop(0, n_a, sent, 0)


def exchange(offsets, slots, x, oz, oy):
    return pl.pallas_call(
        functools.partial(exchange_kernel, oz, oy),
        out_shape=[
            jax.ShapeDtypeStruct((16, 2, 288, 128), jnp.float32),
            jax.ShapeDtypeStruct((768, 128), jnp.float32),
        ],
        in_specs=[
            pl.BlockSpec(memory_space=pltpu.SMEM),
            pl.BlockSpec(memory_space=pltpu.SMEM),
            pl.BlockSpec(memory_space=pl.ANY),
        ],
        out_specs=[pl.BlockSpec(memory_space=pl.ANY), pl.BlockSpec(memory_space=pltpu.VMEM)],
        scratch_shapes=[
            pltpu.VMEM((4, 4, 12, 48, 128), jnp.float32),
            pltpu.VMEM((1, 128), jnp.int32),
            pltpu.SMEM((8, 1, 128), jnp.int32),
            pltpu.VMEM((8, 1, 128), jnp.int32),
            pltpu.VMEM((16 * 144, 128), jnp.float32),
            pltpu.VMEM((16, 4, 4, 9, 4, 128), jnp.float32),
            pltpu.VMEM((16, 4, 4, 9, 4, 128), jnp.float32),
            pltpu.VMEM((16, 2, 288, 128), jnp.float32),
            pltpu.SemaphoreType.DMA((3, 2, 16)),
            pltpu.SemaphoreType.DMA((3, 2, 16)),
            pltpu.SemaphoreType.DMA((8,)),
            pltpu.SemaphoreType.DMA((8,)),
            pltpu.SemaphoreType.DMA((19,)),
            pltpu.SemaphoreType.DMA((4,)),
        ],
        compiler_params=pltpu.CompilerParams(has_side_effects=True, collective_id=3 * (oz - 1) + oy - 1),
        name=f"exchange_{oz}{oy}",
    )(offsets, slots, x)


def per_device(near_null, offsets, owner_slot):
    x = near_null.transpose(0, 1, 3, 4, 2, 5).reshape(4, 4, 12, 48, 128)
    branches = [functools.partial(exchange, oz=oz, oy=oy) for oz in (1, 2, 3) for oy in (1, 2, 3)]
    sites, grams = lax.switch(jnp.sum(offsets * jnp.array([0, 3, 1, 0], jnp.int32)) - 4, branches, offsets, owner_slot.reshape(16), x)
    return finish(grams, sites)


def solution(mesh):
    return jax.shard_map(
        per_device,
        mesh=mesh,
        in_specs=(P("ta", "gz", "gy", None, None, None), P(), P("ta", "gz", "gy", None)),
        out_specs=P(("ta", "gz", "gy"), None, None, None, None, None),
        check_vma=False,
    )
```
